32 devices in a mesh: rep: 1, dp: 32 (over x, y, z, core).
Axes of the slice: x: 2, y: 2, z: 4, core: 2. Of those that a mesh axis runs over, the one named last changes fastest.
Arguments:
- a: bfloat16 [32, 2, 4096, 1280], P(('rep', 'dp'))
- g: bfloat16 [32, 2, 4096, 5120], P(('rep', 'dp'))
Outputs:
- output: bfloat16 [2, 1280, 5120], P('rep')
All inputs are finite; a program needn't handle non-finite values.
Results may differ from the reference program's by a relative error of at most 0.012.
Values are sent between devices in bfloat16 or wider.
A program may use at most 2 GiB of HBM per device.

```python
import jax
import jax.numpy as jnp
from jax import lax

DEVICES = 32
MATRICES = 2
TOKENS = 4096
D = 1280
FF = 5120


def setup_inputs(seed: int = 0, part: int = 0) -> dict:
    ka, kg, ks = (jax.random.fold_in(k, part) for k in jax.random.split(jax.random.key(seed), 3))
    size = 2.0 ** jax.random.uniform(ks, (DEVICES, MATRICES, 1, 1), jnp.float32, -1.0, 1.0)
    a = jax.random.normal(ka, (DEVICES, MATRICES, TOKENS, D), jnp.float32)
    g = size * jax.random.normal(kg, (DEVICES, MATRICES, TOKENS, FF), jnp.float32) * (DEVICES * TOKENS) ** -0.5
    return {"a": a.astype(jnp.bfloat16), "g": g.astype(jnp.bfloat16)}


def reference(a, g):
    def take(so_far, one):
        return so_far + jnp.einsum("ntd,ntf->ndf", *one, preferred_element_type=jnp.float32), None

    return lax.scan(take, jnp.zeros((MATRICES, D, FF), jnp.float32), (a, g))[0].astype(jnp.bfloat16)
```

```python
import functools

import jax
import jax.numpy as jnp
from jax import lax
from jax.experimental import pallas as pl
from jax.experimental.pallas import tpu as pltpu
from jax.sharding import PartitionSpec as P

MESH = pl.DeviceIdType.MESH
F32, BF16 = jnp.float32, jnp.bfloat16
CREDITS = 3
KEPT = 10
S1, S2, S3, S4, S5, S6, S7 = 4, 8, 12, 16, 20, 23, 27
HOP = 4


def kernel(width, stage, a_ref, g_ref, o_ref, aT, ast, gbuf, send0, recv0, mL, mK, sendA, recvA, sendR, sendL, recvR,
           recvL, sendB, recvB, fin, a_sem, g_sem, s0, r0, sA, rA, sR, rR, sL, rL, sB, rB, lc, gBs, gB, gZs, gZ, gAs,
           gA, gCs, gC, credit):
    me = lax.axis_index("dp")
    core, z = lax.rem(me, 2), lax.rem(me // 2, 4)
    y, x = lax.rem(me // 8, 2), me // 16
    partner = me + 1 - 2 * core
    over_x, over_y = me + 16 * (1 - 2 * x), me + 8 * (1 - 2 * y)
    over_A = over_x * (1 - core) + over_y * core
    over_B = over_y * (1 - core) + over_x * core
    al, be = x * (1 - core) + y * core, y * (1 - core) + x * core
    up, down = me + 2, me - 2
    mats, depth, rows = a_ref.shape[1:]
    per = g_ref.shape[3] // width
    chunks = mats * per
    half, quarter, piece, leaf = rows // 2, rows // 4, rows // 8, rows // 16
    mine, keep = core * half, core * half + al * quarter
    end = 1 - z // 3
    is_end = (z == 0) | (z == 3)

    def at(c, first, count):
        cols = pl.ds(pl.multiple_of(lax.rem(c, per) * width, width), width)
        return o_ref.at[c // per, pl.ds(pl.multiple_of(first, leaf), count), cols]

    def rdma(src, dst, ssem, rsem, to):
        return pltpu.make_async_remote_copy(src_ref=src, dst_ref=dst, send_sem=ssem, recv_sem=rsem, device_id={"dp": to},
                                            device_id_type=MESH)

    def by_rows(count, block, f):
        @pl.loop(0, count // block)
        def _(i):
            f(pl.multiple_of(i * block, block))

    blk = leaf

    def load_a(n, k):
        return pltpu.make_async_copy(a_ref.at[0, n, pl.ds(pl.multiple_of(k * stage, stage), stage), :],
                                     ast.at[lax.rem(k, 2)], a_sem.at[lax.rem(k, 2)])

    def load_g(t):
        cols = pl.ds(pl.multiple_of(lax.rem(t, per) * width, width), width)
        return pltpu.make_async_copy(g_ref.at[0, t // per, :, cols], gbuf.at[lax.rem(t, 2)], g_sem.at[lax.rem(t, 2)])

    def transpose_a(n):
        @pl.loop(0, depth // stage)
        def _(k):
            load_a(n, k).wait()
            aT[:, pl.ds(pl.multiple_of(k * stage, stage), stage)] = ast[lax.rem(k, 2)].T

            @pl.when(k + 2 < depth // stage)
            def _():
                load_a(n, k + 2).start()

    def product(t, first):
        return jnp.dot(aT[pl.ds(pl.multiple_of(first, quarter), quarter), :], gbuf[lax.rem(t, 2)],
                       preferred_element_type=F32)

    def copy0(c):
        return rdma(send0.at[lax.rem(c, 2)], recv0.at[lax.rem(c, CREDITS)], s0.at[lax.rem(c, 2)],
                    r0.at[lax.rem(c, CREDITS)], partner)

    def copyA(c):
        return rdma(sendA.at[lax.rem(c, 2)], recvA.at[c], sA.at[lax.rem(c, 2)], rA.at[c], over_A)

    def copyR(c):
        return rdma(sendR.at[lax.rem(c, 2)], recvR.at[c], sR.at[lax.rem(c, 2)], rR.at[c], up)

    def copyL(c):
        return rdma(sendL.at[lax.rem(c, 2)], recvL.at[c], sL.at[lax.rem(c, 2)], rL.at[c], down)

    def copyB(c):
        return rdma(sendB.at[lax.rem(c, 2)], recvB.at[c], sB.at[lax.rem(c, 2)], rB.at[c], over_B)

    def reuse(c, copy):
        @pl.when(c >= 2)
        def _():
            copy(c - 2).wait_send()

    def own_leaf(c):
        return at(c, keep + end * piece + be * leaf, leaf)

    def copy_own(c):
        return pltpu.make_async_copy(fin.at[lax.rem(c, 2)], own_leaf(c), lc.at[lax.rem(c, 2)])

    def give_leaf(c):
        return rdma(fin.at[lax.rem(c, 2)], own_leaf(c), gBs.at[lax.rem(c, 2)], gB.at[c], over_B)

    def take_leaf(c):
        there = at(c, keep + end * piece + (1 - be) * leaf, leaf)
        return rdma(there, there, gBs.at[lax.rem(c, 2)], gB.at[c], over_B)

    def stage1(c):
        copy0(c).wait_recv()
        reuse(c, copyA)

        def leaving(i):
            old = recv0[lax.rem(c, CREDITS), pl.ds(pl.multiple_of((1 - al) * quarter + i, blk), blk), :].astype(F32)
            sendA[lax.rem(c, 2), pl.ds(i, blk), :] = (mL[pl.ds(i, blk), :] + old).astype(BF16)

        by_rows(quarter, blk, leaving)
        copyA(c).start()

        def kept(i):
            old = recv0[lax.rem(c, CREDITS), pl.ds(pl.multiple_of(al * quarter + i, blk), blk), :].astype(F32)
            mK[lax.rem(c, KEPT), pl.ds(i, blk), :] += old

        by_rows(quarter, blk, kept)

        @pl.when(c + CREDITS < chunks)
        def _():
            pl.semaphore_signal(credit, inc=1, device_id={"dp": partner}, device_id_type=MESH)

    def pass_on(c, first, arrived, send, copy):
        reuse(c, copy)

        def add(i):
            total = mK[lax.rem(c, KEPT), pl.ds(first + i, blk), :]
            if arrived is not None:
                total = total + arrived[c, pl.ds(i, blk), :].astype(F32)
            send[lax.rem(c, 2), pl.ds(i, blk), :] = total.astype(BF16)

        by_rows(piece, blk, add)
        copy(c).start()

    def stage2(c):
        copyA(c).wait_recv()

        def add(i):
            mK[lax.rem(c, KEPT), pl.ds(i, blk), :] += recvA[c, pl.ds(i, blk), :].astype(F32)

        by_rows(quarter, blk, add)

        @pl.when(z == 0)
        def _():
            pass_on(c, 0, None, sendR, copyR)

        @pl.when(z == 3)
        def _():
            pass_on(c, piece, None, sendL, copyL)

    def hop_up(c):
        copyR(c).wait_recv()
        pass_on(c, 0, recvR, sendR, copyR)

    def hop_down(c):
        copyL(c).wait_recv()
        pass_on(c, piece, recvL, sendL, copyL)

    def stage3(c):
        pl.when(z == 1)(lambda: hop_up(c))
        pl.when(z == 2)(lambda: hop_down(c))

    def stage4(c):
        pl.when(z == 2)(lambda: hop_up(c))
        pl.when(z == 1)(lambda: hop_down(c))

    def finish_z(c, first, arrived, copy):
        copy(c).wait_recv()
        reuse(c, copyB)

        def out(i):
            total = mK[lax.rem(c, KEPT), pl.ds(pl.multiple_of(first + (1 - be) * leaf, leaf), leaf), :]
            total = total + arrived[c, pl.ds(pl.multiple_of((1 - be) * leaf, leaf), leaf), :].astype(F32)
            sendB[lax.rem(c, 2)] = total.astype(BF16)

        out(0)
        copyB(c).start()
        own = pl.ds(pl.multiple_of(first + be * leaf, leaf), leaf)
        mK[lax.rem(c, KEPT), own, :] += arrived[c, pl.ds(pl.multiple_of(be * leaf, leaf), leaf), :].astype(F32)

    def stage5(c):
        pl.when(z == 3)(lambda: finish_z(c, 0, recvR, copyR))
        pl.when(z == 0)(lambda: finish_z(c, piece, recvL, copyL))

    def stage6(c):
        @pl.when(is_end)
        def _():
            copyB(c).wait_recv()
            reuse(c, give_leaf)
            own = pl.ds(pl.multiple_of(end * piece + be * leaf, leaf), leaf)
            fin[lax.rem(c, 2)] = (mK[lax.rem(c, KEPT), own, :] + recvB[c].astype(F32)).astype(BF16)
            give_leaf(c).start()
            copy_own(c).start()

    def to_z(c, d):
        here = at(c, keep + d * piece, piece)
        return rdma(here, here, gZs.at[d], gZ.at[c, d], up if d else down)

    def to_A(c, d):
        here = at(c, keep + d * piece, piece)
        return rdma(here, here, gAs, gA.at[c, d], over_A)

    def from_A(c, d):
        there = at(c, mine + (1 - al) * quarter + d * piece, piece)
        return rdma(there, there, gAs, gA.at[c, d], over_A)

    def to_core(c, first):
        here = at(c, first, piece)
        return rdma(here, here, gCs, gC, partner)

    def far(d):
        return z if d else 3 - z

    def have(c, d, hop):
        if hop < 3:
            to_z(c, d).start()
        to_A(c, d).start()
        to_core(c, keep + d * piece).start()

    def stage7(hop, c):
        for d in (0, 1):
            @pl.when(far(d) == hop)
            def _(d=d):
                if hop == 0:
                    take_leaf(c).wait_recv()
                    copy_own(c).wait()
                else:
                    to_z(c, d).wait_recv()
                have(c, d, hop)

    def stage8(hop, c):
        for d in (0, 1):
            @pl.when(far(d) == hop)
            def _(d=d):
                from_A(c, d).wait_recv()
                to_core(c, mine + (1 - al) * quarter + d * piece).start()

    stages = [(S1, stage1), (S2, stage2), (S3, stage3), (S4, stage4), (S5, stage5), (S6, stage6)]
    stages += [(S7 + HOP * hop, functools.partial(stage7, hop)) for hop in range(4)]
    stages += [(S7 + HOP * hop + HOP, functools.partial(stage8, hop)) for hop in range(4)]
    last = max(lag for lag, _ in stages) // 4

    def serve(t, q):
        for lag, f in sorted(stages, key=lambda s: -s[0]):
            if lag % 4 == q:
                c = t - lag // 4

                @pl.when((c >= 0) & (c < chunks))
                def _(f=f, c=c):
                    f(c)

    load_a(0, 0).start()
    load_a(0, 1).start()
    load_g(0).start()

    @pl.loop(0, chunks + last)
    def _(t):
        @pl.when(t + 1 < chunks)
        def _():
            load_g(t + 1).start()

        serve(t, 0)

        @pl.when(t < chunks)
        def _():
            @pl.when(lax.rem(t, per) == 0)
            def _():
                transpose_a(t // per)

            @pl.when((lax.rem(t, per) == per - 1) & (t + 1 < chunks))
            def _():
                load_a(t // per + 1, 0).start()
                load_a(t // per + 1, 1).start()

            load_g(t).wait()
            reuse(t, copy0)
            send0[lax.rem(t, 2), pl.ds(0, quarter), :] = product(t, (1 - core) * half).astype(BF16)

        serve(t, 1)

        @pl.when(t < chunks)
        def _():
            send0[lax.rem(t, 2), pl.ds(quarter, quarter), :] = product(t, (1 - core) * half + quarter).astype(BF16)

            @pl.when(t >= CREDITS)
            def _():
                pl.semaphore_wait(credit, 1)

            copy0(t).start()

        serve(t, 2)

        @pl.when(t < chunks)
        def _():
            mL[...] = product(t, mine + (1 - al) * quarter)

        serve(t, 3)

        @pl.when(t < chunks)
        def _():
            mK[lax.rem(t, KEPT)] = product(t, keep)

    def rest(first, count):
        return o_ref.at[:, pl.ds(pl.multiple_of(first, leaf), count), :]

    for c in range(chunks - 2, chunks):
        copy0(c).wait_send()
        copyA(c).wait_send()
        pl.when(z < 3)(lambda: copyR(c).wait_send())
        pl.when(z > 0)(lambda: copyL(c).wait_send())

        @pl.when(is_end)
        def _(c=c):
            copyB(c).wait_send()
            give_leaf(c).wait_send()

    for d in (0, 1):
        @pl.when(far(d) < 3)
        def _(d=d):
            some = rest(keep + d * piece, piece)
            rdma(some, some, gZs.at[d], gC, partner).wait_send()

    some = rest(keep, quarter)
    rdma(some, some, gAs, gC, over_A).wait_send()
    some = rest(mine, half)
    rdma(some, some, gCs, gC, partner).wait_send()
    some = rest((1 - core) * half, half)
    rdma(some, some, gCs, gC, partner).wait_recv()


def solution(mesh, width=512, stage=512):
    def step(a, g):
        mats, depth, rows = a.shape[1:]
        columns = g.shape[3]
        chunks = mats * (columns // width)
        half, quarter, piece, leaf = rows // 2, rows // 4, rows // 8, rows // 16
        dma = pltpu.SemaphoreType.DMA
        return pl.pallas_call(
            functools.partial(kernel, width, stage),
            out_shape=jax.ShapeDtypeStruct((mats, rows, columns), BF16),
            in_specs=[pl.BlockSpec(memory_space=pl.ANY)] * 2,
            out_specs=pl.BlockSpec(memory_space=pl.ANY),
            scratch_shapes=[
                pltpu.VMEM((rows, depth), BF16),
                pltpu.VMEM((2, stage, rows), BF16),
                pltpu.VMEM((2, depth, width), BF16),
                pltpu.VMEM((2, half, width), BF16),
                pltpu.VMEM((CREDITS, half, width), BF16),
                pltpu.VMEM((quarter, width), F32),
                pltpu.VMEM((KEPT, quarter, width), F32),
                pltpu.VMEM((2, quarter, width), BF16),
                pltpu.VMEM((chunks, quarter, width), BF16),
                pltpu.VMEM((2, piece, width), BF16),
                pltpu.VMEM((2, piece, width), BF16),
                pltpu.VMEM((chunks, piece, width), BF16),
                pltpu.VMEM((chunks, piece, width), BF16),
                pltpu.VMEM((2, leaf, width), BF16),
                pltpu.VMEM((chunks, leaf, width), BF16),
                pltpu.VMEM((2, leaf, width), BF16),
                dma((2,)), dma((2,)), dma((2,)), dma((CREDITS,)), dma((2,)), dma((chunks,)), dma((2,)), dma((chunks,)),
                dma((2,)), dma((chunks,)), dma((2,)), dma((chunks,)), dma((2,)), dma((2,)), dma((chunks,)), dma((2,)),
                dma((chunks, 2)), dma, dma((chunks, 2)), dma, dma, pltpu.SemaphoreType.REGULAR,
            ],
            compiler_params=pltpu.CompilerParams(has_side_effects=True, vmem_limit_bytes=66 * 1000 * 1000),
        )(a, g)

    return jax.shard_map(step, mesh=mesh, in_specs=(P(("rep", "dp")), P(("rep", "dp"))), out_specs=P("rep"),
                         check_vma=False)
```

```python
import functools

import jax
import jax.numpy as jnp
from jax import lax
from jax.experimental import pallas as pl
from jax.experimental.pallas import tpu as pltpu
from jax.sharding import PartitionSpec as P

MESH = pl.DeviceIdType.MESH
F32, BF16 = jnp.float32, jnp.bfloat16
CREDITS = 4
KEPT = 10
LOADS = 6
S1, S2, S3, S4, S5, S6, S7 = 2, 5, 9, 12, 15, 17, 20
HOP = 5


def kernel(width, stage, a_ref, g_ref, o_ref, aT, ast, gbuf, send0, recv0, mL, mK, sendA, recvA, sendR, sendL, sendB,
           recvB, a_sem, g_sem, s0, r0, sA, rA, sR, rR, sL, rL, sB, rB, gBs, gB, gZs, gZ, gAs, gA, gCs, gC, credit):
    me = lax.axis_index("dp")
    core, z = lax.rem(me, 2), lax.rem(me // 2, 4)
    y, x = lax.rem(me // 8, 2), me // 16
    partner = me + 1 - 2 * core
    over_x, over_y = me + 16 * (1 - 2 * x), me + 8 * (1 - 2 * y)
    over_A = over_x * (1 - core) + over_y * core
    over_B = over_y * (1 - core) + over_x * core
    al, be = x * (1 - core) + y * core, y * (1 - core) + x * core
    up, down = me + 2, me - 2
    mats, depth, rows = a_ref.shape[1:]
    per = g_ref.shape[3] // width
    chunks = mats * per
    half, quarter, piece, leaf = rows // 2, rows // 4, rows // 8, rows // 16
    mine, keep = core * half, core * half + al * quarter
    end = 1 - z // 3
    is_end = (z == 0) | (z == 3)

    def at(c, first, count):
        return o_ref.at[index(c, first, count)]

    def index(c, first, count):
        cols = pl.ds(pl.multiple_of(lax.rem(c, per) * width, width), width)
        return c // per, pl.ds(pl.multiple_of(first, leaf), count), cols

    def rdma(src, dst, ssem, rsem, to):
        return pltpu.make_async_remote_copy(src_ref=src, dst_ref=dst, send_sem=ssem, recv_sem=rsem, device_id={"dp": to},
                                            device_id_type=MESH)

    def by_rows(count, block, f):
        @pl.loop(0, count // block)
        def _(i):
            f(pl.multiple_of(i * block, block))

    blk = leaf

    def load_a(n, k):
        return pltpu.make_async_copy(a_ref.at[0, n, pl.ds(pl.multiple_of(k * stage, stage), stage), :],
                                     ast.at[lax.rem(k, LOADS)], a_sem.at[lax.rem(k, LOADS)])

    def load_g(t):
        cols = pl.ds(pl.multiple_of(lax.rem(t, per) * width, width), width)
        return pltpu.make_async_copy(g_ref.at[0, t // per, :, cols], gbuf.at[lax.rem(t, 2)], g_sem.at[lax.rem(t, 2)])

    def start_a(n):
        for k in range(min(LOADS, depth // stage)):
            load_a(n, k).start()

    def transpose_a(n):
        @pl.loop(0, depth // stage)
        def _(k):
            load_a(n, k).wait()
            block = ast[lax.rem(k, LOADS)].T
            for h in (0, 1):
                for j in (0, 1):
                    away = jnp.abs(core - h)
                    to = away * j + (1 - away) * (3 - jnp.abs(al - j))
                    rows_to = pl.ds(pl.multiple_of(to * quarter, quarter), quarter)
                    first = h * half + j * quarter
                    aT[rows_to, pl.ds(pl.multiple_of(k * stage, stage), stage)] = block[first:first + quarter]

            @pl.when(k + LOADS < depth // stage)
            def _():
                load_a(n, k + LOADS).start()

    def product(t, first):
        return jnp.dot(aT[first:first + half, :], gbuf[lax.rem(t, 2)], preferred_element_type=F32)

    def copy0(c):
        return rdma(send0.at[lax.rem(c, 2)], recv0.at[lax.rem(c, CREDITS)], s0.at[lax.rem(c, 2)],
                    r0.at[lax.rem(c, CREDITS)], partner)

    def copyA(c):
        return rdma(sendA.at[lax.rem(c, 2)], recvA.at[c], sA.at[lax.rem(c, 2)], rA.at[c], over_A)

    def copyR(c):
        return rdma(sendR.at[lax.rem(c, 2)], at(c, keep, piece), sR.at[lax.rem(c, 2)], rR.at[c], up)

    def copyL(c):
        return rdma(sendL.at[lax.rem(c, 2)], at(c, keep + piece, piece), sL.at[lax.rem(c, 2)], rL.at[c], down)

    def copyB(c):
        return rdma(sendB.at[lax.rem(c, 2)], recvB.at[c], sB.at[lax.rem(c, 2)], rB.at[c], over_B)

    def reuse(c, copy):
        @pl.when(c >= 2)
        def _():
            copy(c - 2).wait_send()

    def give_leaf(c):
        own = at(c, keep + end * piece + be * leaf, leaf)
        return rdma(own, own, gBs, gB.at[c], over_B)

    def take_leaf(c):
        there = at(c, keep + end * piece + (1 - be) * leaf, leaf)
        return rdma(there, there, gBs, gB.at[c], over_B)

    def stage1(c):
        copy0(c).wait_recv()
        reuse(c, copyA)

        def leaving(i):
            old = recv0[lax.rem(c, CREDITS), pl.ds(pl.multiple_of((1 - al) * quarter + i, blk), blk), :].astype(F32)
            sendA[lax.rem(c, 2), pl.ds(i, blk), :] = (mL[pl.ds(i, blk), :] + old).astype(BF16)

        by_rows(quarter, blk, leaving)
        copyA(c).start()

        def kept(i):
            old = recv0[lax.rem(c, CREDITS), pl.ds(pl.multiple_of(al * quarter + i, blk), blk), :].astype(F32)
            mK[lax.rem(c, KEPT), pl.ds(i, blk), :] += old

        by_rows(quarter, blk, kept)

        @pl.when(c + CREDITS < chunks)
        def _():
            pl.semaphore_signal(credit, inc=1, device_id={"dp": partner}, device_id_type=MESH)

    def pass_on(c, first, arrived, send, copy):
        reuse(c, copy)

        def add(i):
            total = mK[lax.rem(c, KEPT), pl.ds(first + i, blk), :]
            if arrived:
                total = total + o_ref[index(c, keep + first + i, blk)].astype(F32)
            send[lax.rem(c, 2), pl.ds(i, blk), :] = total.astype(BF16)

        by_rows(piece, blk, add)
        copy(c).start()

    def stage2(c):
        copyA(c).wait_recv()

        def add(i):
            mK[lax.rem(c, KEPT), pl.ds(i, blk), :] += recvA[c, pl.ds(i, blk), :].astype(F32)

        by_rows(quarter, blk, add)

        @pl.when(z == 0)
        def _():
            pass_on(c, 0, False, sendR, copyR)

        @pl.when(z == 3)
        def _():
            pass_on(c, piece, False, sendL, copyL)

    def hop_up(c):
        copyR(c).wait_recv()
        pass_on(c, 0, True, sendR, copyR)

    def hop_down(c):
        copyL(c).wait_recv()
        pass_on(c, piece, True, sendL, copyL)

    def stage3(c):
        pl.when(z == 1)(lambda: hop_up(c))
        pl.when(z == 2)(lambda: hop_down(c))

    def stage4(c):
        pl.when(z == 2)(lambda: hop_up(c))
        pl.when(z == 1)(lambda: hop_down(c))

    def finish_z(c, first, copy):
        copy(c).wait_recv()
        reuse(c, copyB)
        away = first + (1 - be) * leaf
        total = mK[lax.rem(c, KEPT), pl.ds(pl.multiple_of(away, leaf), leaf), :]
        sendB[lax.rem(c, 2)] = (total + o_ref[index(c, keep + away, leaf)].astype(F32)).astype(BF16)
        copyB(c).start()
        stay = first + be * leaf
        own = pl.ds(pl.multiple_of(stay, leaf), leaf)
        mK[lax.rem(c, KEPT), own, :] += o_ref[index(c, keep + stay, leaf)].astype(F32)

    def stage5(c):
        pl.when(z == 3)(lambda: finish_z(c, 0, copyR))
        pl.when(z == 0)(lambda: finish_z(c, piece, copyL))

    def stage6(c):
        @pl.when(is_end)
        def _():
            copyB(c).wait_recv()
            stay = end * piece + be * leaf
            total = mK[lax.rem(c, KEPT), pl.ds(pl.multiple_of(stay, leaf), leaf), :] + recvB[c].astype(F32)
            o_ref[index(c, keep + stay, leaf)] = total.astype(BF16)
            give_leaf(c).start()

    def to_z(c, d):
        here = at(c, keep + d * piece, piece)
        return rdma(here, here, gZs.at[d], gZ.at[c, d], up if d else down)

    def to_A(c, d):
        here = at(c, keep + d * piece, piece)
        return rdma(here, here, gAs, gA.at[c, d], over_A)

    def from_A(c, d):
        there = at(c, mine + (1 - al) * quarter + d * piece, piece)
        return rdma(there, there, gAs, gA.at[c, d], over_A)

    def to_core(c, first):
        here = at(c, first, piece)
        return rdma(here, here, gCs, gC, partner)

    def far(d):
        return z if d else 3 - z

    def have(c, d, hop):
        if hop < 3:
            to_z(c, d).start()
        to_A(c, d).start()
        to_core(c, keep + d * piece).start()

    def stage7(hop, c):
        for d in (0, 1):
            @pl.when(far(d) == hop)
            def _(d=d):
                if hop == 0:
                    take_leaf(c).wait_recv()
                else:
                    to_z(c, d).wait_recv()
                have(c, d, hop)

    def stage8(hop, c):
        for d in (0, 1):
            @pl.when(far(d) == hop)
            def _(d=d):
                from_A(c, d).wait_recv()
                to_core(c, mine + (1 - al) * quarter + d * piece).start()

    stages = [(S1, stage1), (S2, stage2), (S3, stage3), (S4, stage4), (S5, stage5), (S6, stage6)]
    stages += [(S7 + HOP * hop, functools.partial(stage7, hop)) for hop in range(4)]
    stages += [(S7 + HOP * hop + HOP, functools.partial(stage8, hop)) for hop in range(4)]
    last = max(lag for lag, _ in stages) // 2

    def serve(t, q):
        for lag, f in sorted(stages, key=lambda s: s[0]):
            if lag % 2 == q:
                c = t - lag // 2

                @pl.when((c >= 0) & (c < chunks))
                def _(f=f, c=c):
                    f(c)

    start_a(0)
    load_g(0).start()

    @pl.loop(0, chunks + last)
    def _(t):
        @pl.when(t + 1 < chunks)
        def _():
            load_g(t + 1).start()

        serve(t, 0)

        @pl.when(t < chunks)
        def _():
            @pl.when(lax.rem(t, per) == 0)
            def _():
                transpose_a(t // per)

            @pl.when((lax.rem(t, per) == per - 1) & (t + 1 < chunks))
            def _():
                start_a(t // per + 1)

            load_g(t).wait()
            reuse(t, copy0)
            send0[lax.rem(t, 2)] = product(t, 0).astype(BF16)

            @pl.when(t >= CREDITS)
            def _():
                pl.semaphore_wait(credit, 1)

            copy0(t).start()

        serve(t, 1)

        @pl.when(t < chunks)
        def _():
            both = product(t, half)
            mL[...] = both[:quarter]
            mK[lax.rem(t, KEPT)] = both[quarter:]

    def rest(first, count):
        return o_ref.at[:, pl.ds(pl.multiple_of(first, leaf), count), :]

    for c in range(chunks - 2, chunks):
        copy0(c).wait_send()
        copyA(c).wait_send()
        pl.when(z < 3)(lambda: copyR(c).wait_send())
        pl.when(z > 0)(lambda: copyL(c).wait_send())

        @pl.when(is_end)
        def _(c=c):
            copyB(c).wait_send()

    @pl.when(is_end)
    def _():
        some = rest(keep, leaf)
        rdma(some, some, gBs, gC, over_B).wait_send()

    for d in (0, 1):
        @pl.when(far(d) < 3)
        def _(d=d):
            some = rest(keep + d * piece, piece)
            rdma(some, some, gZs.at[d], gC, partner).wait_send()

    some = rest(keep, quarter)
    rdma(some, some, gAs, gC, over_A).wait_send()
    some = rest(mine, half)
    rdma(some, some, gCs, gC, partner).wait_send()
    some = rest((1 - core) * half, half)
    rdma(some, some, gCs, gC, partner).wait_recv()


def solution(mesh, width=256, stage=256):
    def step(a, g):
        mats, depth, rows = a.shape[1:]
        columns = g.shape[3]
        chunks = mats * (columns // width)
        half, quarter, piece, leaf = rows // 2, rows // 4, rows // 8, rows // 16
        dma = pltpu.SemaphoreType.DMA
        return pl.pallas_call(
            functools.partial(kernel, width, stage),
            out_shape=pltpu.VMEM((mats, rows, columns), BF16),
            in_specs=[pl.BlockSpec(memory_space=pl.ANY)] * 2,
            out_specs=pl.BlockSpec(memory_space=pltpu.VMEM),
            scratch_shapes=[
                pltpu.VMEM((rows, depth), BF16),
                pltpu.VMEM((LOADS, stage, rows), BF16),
                pltpu.VMEM((2, depth, width), BF16),
                pltpu.VMEM((2, half, width), BF16),
                pltpu.VMEM((CREDITS, half, width), BF16),
                pltpu.VMEM((quarter, width), F32),
                pltpu.VMEM((KEPT, quarter, width), F32),
                pltpu.VMEM((2, quarter, width), BF16),
                pltpu.VMEM((chunks, quarter, width), BF16),
                pltpu.VMEM((2, piece, width), BF16),
                pltpu.VMEM((2, piece, width), BF16),
                pltpu.VMEM((2, leaf, width), BF16),
                pltpu.VMEM((chunks, leaf, width), BF16),
                dma((LOADS,)), dma((2,)), dma((2,)), dma((CREDITS,)), dma((2,)), dma((chunks,)), dma((2,)),
                dma((chunks,)), dma((2,)), dma((chunks,)), dma((2,)), dma((chunks,)), dma, dma((chunks,)), dma((2,)),
                dma((chunks, 2)), dma, dma((chunks, 2)), dma, dma, pltpu.SemaphoreType.REGULAR,
            ],
            compiler_params=pltpu.CompilerParams(has_side_effects=True, vmem_limit_bytes=40 * 1000 * 1000),
        )(a, g)

    return jax.shard_map(step, mesh=mesh, in_specs=(P(("rep", "dp")), P(("rep", "dp"))), out_specs=P("rep"),
                         check_vma=False)
```

```python
import functools

import jax
import jax.numpy as jnp
from jax import lax
from jax.experimental import pallas as pl
from jax.experimental.pallas import tpu as pltpu
from jax.sharding import PartitionSpec as P

MESH = pl.DeviceIdType.MESH
F32, BF16 = jnp.float32, jnp.bfloat16
CREDITS = 8
KEPT = 16
LOADS = 6
S1, S2, S3, S4, S5, S6, S7 = 2, 5, 9, 12, 15, 17, 20
HOP = 5


def kernel(width, stage, a_ref, g_ref, o_ref, aT, ast, gbuf, send0, recv0, mL, mK, sendA, recvA, sendR, sendL, sendB,
           recvB, a_sem, g_sem, s0, r0, sA, rA, sR, rR, sL, rL, sB, rB, gBs, gB, gZs, gZ, gAs, gA, gCs, gC, credit):
    me = lax.axis_index("dp")
    core, z = lax.rem(me, 2), lax.rem(me // 2, 4)
    y, x = lax.rem(me // 8, 2), me // 16
    partner = me + 1 - 2 * core
    over_x, over_y = me + 16 * (1 - 2 * x), me + 8 * (1 - 2 * y)
    over_A = over_x * (1 - core) + over_y * core
    over_B = over_y * (1 - core) + over_x * core
    al, be = x * (1 - core) + y * core, y * (1 - core) + x * core
    up, down = me + 2, me - 2
    mats, depth, rows = a_ref.shape[1:]
    per = g_ref.shape[3] // width
    chunks = mats * per
    half, quarter, piece, leaf = rows // 2, rows // 4, rows // 8, rows // 16
    mine, keep = core * half, core * half + al * quarter
    end = 1 - z // 3
    is_end = (z == 0) | (z == 3)

    def at(c, first, count):
        return o_ref.at[index(c, first, count)]

    def place(c):
        n = c // per if isinstance(c, int) else sum((c >= m * per).astype(jnp.int32) for m in range(1, mats))
        return n, pl.ds(pl.multiple_of((c - n * per) * width, width), width)

    def index(c, first, count):
        n, cols = place(c)
        return n, pl.ds(pl.multiple_of(first, leaf), count), cols

    def rdma(src, dst, ssem, rsem, to):
        return pltpu.make_async_remote_copy(src_ref=src, dst_ref=dst, send_sem=ssem, recv_sem=rsem, device_id={"dp": to},
                                            device_id_type=MESH)

    def load_a(n, k):
        return pltpu.make_async_copy(a_ref.at[0, n, pl.ds(pl.multiple_of(k * stage, stage), stage), :],
                                     ast.at[lax.rem(k, LOADS)], a_sem.at[lax.rem(k, LOADS)])

    def load_g(t):
        n, cols = place(t)
        return pltpu.make_async_copy(g_ref.at[0, n, :, cols], gbuf.at[lax.rem(t, 2)], g_sem.at[lax.rem(t, 2)])

    def start_a(n):
        for k in range(min(LOADS, depth // stage)):
            load_a(n, k).start()

    def transpose_a(n):
        @pl.loop(0, depth // stage)
        def _(k):
            load_a(n, k).wait()
            block = ast[lax.rem(k, LOADS)].T
            for h in (0, 1):
                for j in (0, 1):
                    away = jnp.abs(core - h)
                    to = away * j + (1 - away) * (3 - jnp.abs(al - j))
                    rows_to = pl.ds(pl.multiple_of(to * quarter, quarter), quarter)
                    first = h * half + j * quarter
                    aT[rows_to, pl.ds(pl.multiple_of(k * stage, stage), stage)] = block[first:first + quarter]

            @pl.when(k + LOADS < depth // stage)
            def _():
                load_a(n, k + LOADS).start()

    def product(t, first):
        return jnp.dot(aT[first:first + half, :], gbuf[lax.rem(t, 2)], preferred_element_type=F32)

    def copy0(c):
        return rdma(send0.at[lax.rem(c, 2)], recv0.at[lax.rem(c, CREDITS)], s0.at[lax.rem(c, 2)],
                    r0.at[lax.rem(c, CREDITS)], partner)

    def copyA(c):
        return rdma(sendA.at[lax.rem(c, 2)], recvA.at[c], sA.at[lax.rem(c, 2)], rA.at[c], over_A)

    def copyR(c):
        return rdma(sendR.at[lax.rem(c, 2)], at(c, keep, piece), sR.at[lax.rem(c, 2)], rR.at[c], up)

    def copyL(c):
        return rdma(sendL.at[lax.rem(c, 2)], at(c, keep + piece, piece), sL.at[lax.rem(c, 2)], rL.at[c], down)

    def copyB(c):
        return rdma(sendB.at[lax.rem(c, 2)], recvB.at[c], sB.at[lax.rem(c, 2)], rB.at[c], over_B)

    def reuse(c, copy):
        @pl.when(c >= 2)
        def _():
            copy(c - 2).wait_send()

    def give_leaf(c):
        own = at(c, keep + end * piece + be * leaf, leaf)
        return rdma(own, own, gBs, gB.at[c], over_B)

    def take_leaf(c):
        there = at(c, keep + end * piece + (1 - be) * leaf, leaf)
        return rdma(there, there, gBs, gB.at[c], over_B)

    def stage1(c):
        copy0(c).wait_recv()
        reuse(c, copyA)
        for i in (0, piece):
            old = recv0[lax.rem(c, CREDITS), pl.ds(pl.multiple_of((1 - al) * quarter + i, piece), piece), :]
            sendA[lax.rem(c, 2), i:i + piece, :] = (mL[i:i + piece, :] + old.astype(F32)).astype(BF16)
        copyA(c).start()

    def total(c, i):
        old = recv0[lax.rem(c, CREDITS), pl.ds(pl.multiple_of(al * quarter + i, piece), piece), :]
        here = mK[lax.rem(c, KEPT), i:i + piece, :] + old.astype(F32)
        return here + recvA[c, i:i + piece, :].astype(F32)

    def first_hop(c, i, send, copy):
        reuse(c, copy)
        send[lax.rem(c, 2)] = total(c, i).astype(BF16)
        copy(c).start()
        mK[lax.rem(c, KEPT), piece - i:2 * piece - i, :] = total(c, piece - i)

    def stage2(c):
        copyA(c).wait_recv()
        pl.when(z == 0)(lambda: first_hop(c, 0, sendR, copyR))
        pl.when(z == 3)(lambda: first_hop(c, piece, sendL, copyL))

        @pl.when((z == 1) | (z == 2))
        def _():
            for i in (0, piece):
                mK[lax.rem(c, KEPT), i:i + piece, :] = total(c, i)

        @pl.when(c + CREDITS < chunks)
        def _():
            pl.semaphore_signal(credit, inc=1, device_id={"dp": partner}, device_id_type=MESH)

    def pass_on(c, first, send, copy):
        copy(c).wait_recv()
        reuse(c, copy)
        here = mK[lax.rem(c, KEPT), first:first + piece, :]
        send[lax.rem(c, 2)] = (here + o_ref[index(c, keep + first, piece)].astype(F32)).astype(BF16)
        copy(c).start()

    def hop_up(c):
        pass_on(c, 0, sendR, copyR)

    def hop_down(c):
        pass_on(c, piece, sendL, copyL)

    def stage3(c):
        pl.when(z == 1)(lambda: hop_up(c))
        pl.when(z == 2)(lambda: hop_down(c))

    def stage4(c):
        pl.when(z == 2)(lambda: hop_up(c))
        pl.when(z == 1)(lambda: hop_down(c))

    def finish_z(c, first, copy):
        copy(c).wait_recv()
        reuse(c, copyB)
        away = first + (1 - be) * leaf
        total = mK[lax.rem(c, KEPT), pl.ds(pl.multiple_of(away, leaf), leaf), :]
        sendB[lax.rem(c, 2)] = (total + o_ref[index(c, keep + away, leaf)].astype(F32)).astype(BF16)
        copyB(c).start()
        stay = first + be * leaf
        own = pl.ds(pl.multiple_of(stay, leaf), leaf)
        mK[lax.rem(c, KEPT), own, :] += o_ref[index(c, keep + stay, leaf)].astype(F32)

    def stage5(c):
        pl.when(z == 3)(lambda: finish_z(c, 0, copyR))
        pl.when(z == 0)(lambda: finish_z(c, piece, copyL))

    def stage6(c):
        @pl.when(is_end)
        def _():
            copyB(c).wait_recv()
            stay = end * piece + be * leaf
            total = mK[lax.rem(c, KEPT), pl.ds(pl.multiple_of(stay, leaf), leaf), :] + recvB[c].astype(F32)
            o_ref[index(c, keep + stay, leaf)] = total.astype(BF16)
            give_leaf(c).start()

    def to_z(c, d):
        here = at(c, keep + d * piece, piece)
        return rdma(here, here, gZs.at[d], gZ.at[c, d], up if d else down)

    def to_A(c, d):
        here = at(c, keep + d * piece, piece)
        return rdma(here, here, gAs, gA.at[c, d], over_A)

    def from_A(c, d):
        there = at(c, mine + (1 - al) * quarter + d * piece, piece)
        return rdma(there, there, gAs, gA.at[c, d], over_A)

    def to_core(c):
        here = at(c, mine, half)
        return rdma(here, here, gCs, gC, partner)

    def far(d):
        return z if d else 3 - z

    def have(c, d, hop):
        if hop < 3:
            to_z(c, d).start()
        to_A(c, d).start()

    def stage7(hop, c):
        for d in (0, 1):
            @pl.when(far(d) == hop)
            def _(d=d):
                if hop == 0:
                    take_leaf(c).wait_recv()
                else:
                    to_z(c, d).wait_recv()
                have(c, d, hop)

    def stage8(hop, c):
        for d in (0, 1):
            @pl.when(far(d) == hop)
            def _(d=d):
                from_A(c, d).wait_recv()

        if hop >= 2:
            @pl.when((jnp.maximum(far(0), far(1)) == hop))
            def _():
                to_core(c).start()

    stages = [(S1, stage1), (S2, stage2), (S3, stage3), (S4, stage4), (S5, stage5), (S6, stage6)]
    stages += [(S7 + HOP * hop, functools.partial(stage7, hop)) for hop in range(4)]
    stages += [(S7 + HOP * hop + HOP, functools.partial(stage8, hop)) for hop in range(4)]
    last = max(lag for lag, _ in stages) // 2

    def serve(t, q):
        for lag, f in sorted(stages, key=lambda s: s[0]):
            if lag % 2 == q:
                c = t - lag // 2

                @pl.when((c >= 0) & (c < chunks))
                def _(f=f, c=c):
                    f(c)

    start_a(0)
    load_g(0).start()
    barrier = pltpu.get_barrier_semaphore()
    for other in (partner, over_A, over_B):
        pl.semaphore_signal(barrier, inc=1, device_id={"dp": other}, device_id_type=MESH)

    @pl.when(z < 3)
    def _():
        pl.semaphore_signal(barrier, inc=1, device_id={"dp": up}, device_id_type=MESH)

    @pl.when(z > 0)
    def _():
        pl.semaphore_signal(barrier, inc=1, device_id={"dp": down}, device_id_type=MESH)

    transpose_a(0)
    pl.semaphore_wait(barrier, 3 + (z < 3).astype(jnp.int32) + (z > 0).astype(jnp.int32))

    @pl.loop(0, chunks + last)
    def _(t):
        @pl.when(t + 1 < chunks)
        def _():
            load_g(t + 1).start()

        serve(t, 0)

        @pl.when(t < chunks)
        def _():
            for n in range(1, mats):
                pl.when(t == n * per)(functools.partial(transpose_a, n))
                pl.when(t == n * per - 1)(functools.partial(start_a, n))

            load_g(t).wait()
            reuse(t, copy0)
            send0[lax.rem(t, 2)] = product(t, 0).astype(BF16)

            @pl.when(t >= CREDITS)
            def _():
                pl.semaphore_wait(credit, 1)

            copy0(t).start()

        serve(t, 1)

        @pl.when(t < chunks)
        def _():
            both = product(t, half)
            mL[...] = both[:quarter]
            mK[lax.rem(t, KEPT)] = both[quarter:]

    def rest(first, count):
        return o_ref.at[:, pl.ds(pl.multiple_of(first, leaf), count), :]

    for c in range(chunks - 2, chunks):
        copy0(c).wait_send()
        copyA(c).wait_send()
        pl.when(z < 3)(lambda: copyR(c).wait_send())
        pl.when(z > 0)(lambda: copyL(c).wait_send())

        @pl.when(is_end)
        def _(c=c):
            copyB(c).wait_send()

    @pl.when(is_end)
    def _():
        some = rest(keep, leaf)
        rdma(some, some, gBs, gC, over_B).wait_send()

    for d in (0, 1):
        @pl.when(far(d) < 3)
        def _(d=d):
            some = rest(keep + d * piece, piece)
            rdma(some, some, gZs.at[d], gC, partner).wait_send()

    some = rest(keep, quarter)
    rdma(some, some, gAs, gC, over_A).wait_send()
    some = rest(mine, half)
    rdma(some, some, gCs, gC, partner).wait_send()
    some = rest((1 - core) * half, half)
    rdma(some, some, gCs, gC, partner).wait_recv()


def solution(mesh, width=256, stage=256):
    def step(a, g):
        mats, depth, rows = a.shape[1:]
        columns = g.shape[3]
        chunks = mats * (columns // width)
        half, quarter, piece, leaf = rows // 2, rows // 4, rows // 8, rows // 16
        dma = pltpu.SemaphoreType.DMA
        return pl.pallas_call(
            functools.partial(kernel, width, stage),
            out_shape=pltpu.VMEM((mats, rows, columns), BF16),
            in_specs=[pl.BlockSpec(memory_space=pl.ANY)] * 2,
            out_specs=pl.BlockSpec(memory_space=pltpu.VMEM),
            scratch_shapes=[
                pltpu.VMEM((rows, depth), BF16),
                pltpu.VMEM((LOADS, stage, rows), BF16),
                pltpu.VMEM((2, depth, width), BF16),
                pltpu.VMEM((2, half, width), BF16),
                pltpu.VMEM((CREDITS, half, width), BF16),
                pltpu.VMEM((quarter, width), F32),
                pltpu.VMEM((KEPT, quarter, width), F32),
                pltpu.VMEM((2, quarter, width), BF16),
                pltpu.VMEM((chunks, quarter, width), BF16),
                pltpu.VMEM((2, piece, width), BF16),
                pltpu.VMEM((2, piece, width), BF16),
                pltpu.VMEM((2, leaf, width), BF16),
                pltpu.VMEM((chunks, leaf, width), BF16),
                dma((LOADS,)), dma((2,)), dma((2,)), dma((CREDITS,)), dma((2,)), dma((chunks,)), dma((2,)),
                dma((chunks,)), dma((2,)), dma((chunks,)), dma((2,)), dma((chunks,)), dma, dma((chunks,)), dma((2,)),
                dma((chunks, 2)), dma, dma((chunks, 2)), dma, dma, pltpu.SemaphoreType.REGULAR,
            ],
            compiler_params=pltpu.CompilerParams(collective_id=0, has_side_effects=True, vmem_limit_bytes=40 * 1000 * 1000),
        )(a, g)

    return jax.shard_map(step, mesh=mesh, in_specs=(P(("rep", "dp")), P(("rep", "dp"))), out_specs=P("rep"),
                         check_vma=False)
```

```python
import functools

import jax
import jax.numpy as jnp
from jax import lax
from jax.experimental import pallas as pl
from jax.experimental.pallas import tpu as pltpu
from jax.sharding import PartitionSpec as P

MESH = pl.DeviceIdType.MESH
F32, BF16 = jnp.float32, jnp.bfloat16
CREDITS = 8
KEPT = 16
LOADS = 8
S1, S2, S3, S4, S5, S6 = 2, 5, 9, 12, 15, 17
S7 = 20, 25, 30, 36
S8 = 27, 32, 35, 46


def wide(c):
    return (lax.rem(c, 4) == 2) & (c < 22)


def kernel(width, stage, a_ref, g_ref, o_ref, aT, ast, gbuf, send0, recv0, mL, mK, sendA, recvA, sendR, sendL, sendB,
           recvB, a_sem, g_sem, s0, r0, sA, rA, sR, rR, sL, rL, sB, rB, gBs, gB, gZs, gZ, gNs, gAs, gA, gCs, gC, credit):
    me = lax.axis_index("dp")
    core, z = lax.rem(me, 2), lax.rem(me // 2, 4)
    y, x = lax.rem(me // 8, 2), me // 16
    partner = me + 1 - 2 * core
    over_x, over_y = me + 16 * (1 - 2 * x), me + 8 * (1 - 2 * y)
    over_A = over_x * (1 - core) + over_y * core
    over_B = over_y * (1 - core) + over_x * core
    al, be = x * (1 - core) + y * core, y * (1 - core) + x * core
    up, down = me + 2, me - 2
    mats, depth, rows = a_ref.shape[1:]
    per = g_ref.shape[3] // width
    chunks = mats * per
    half, quarter, piece, leaf = rows // 2, rows // 4, rows // 8, rows // 16
    mine, keep = core * half, core * half + al * quarter
    end = 1 - z // 3
    is_end = (z == 0) | (z == 3)

    def at(c, first, count):
        return o_ref.at[index(c, first, count)]

    def place(c):
        n = c // per if isinstance(c, int) else sum((c >= m * per).astype(jnp.int32) for m in range(1, mats))
        return n, pl.ds(pl.multiple_of((c - n * per) * width, width), width)

    def index(c, first, count):
        n, cols = place(c)
        return n, pl.ds(pl.multiple_of(first, leaf), count), cols

    def rdma(src, dst, ssem, rsem, to):
        return pltpu.make_async_remote_copy(src_ref=src, dst_ref=dst, send_sem=ssem, recv_sem=rsem, device_id={"dp": to},
                                            device_id_type=MESH)

    blocks = depth // stage

    def load_a(n, i):
        late = int(i >= blocks) if isinstance(i, int) else (i >= blocks).astype(jnp.int32)
        k = i - late * blocks
        cols = pl.ds(pl.multiple_of((core * late + (1 - core) * (1 - late)) * half, half), half)
        slot = lax.rem(i, LOADS)
        return pltpu.make_async_copy(a_ref.at[0, n, pl.ds(pl.multiple_of(k * stage, stage), stage), cols], ast.at[slot],
                                     a_sem.at[slot])

    def load_g(t):
        n, cols = place(t)
        return pltpu.make_async_copy(g_ref.at[0, n, :, cols], gbuf.at[lax.rem(t, 2)], g_sem.at[lax.rem(t, 2)])

    def start_a(n):
        for i in range(min(LOADS, 2 * blocks)):
            load_a(n, i).start()

    def transpose_a(n, late):
        @pl.loop(late * blocks, (late + 1) * blocks)
        def _(i):
            load_a(n, i).wait()
            block = ast[lax.rem(i, LOADS)].T
            cols = pl.ds(pl.multiple_of((i - late * blocks) * stage, stage), stage)
            if late:
                for j in (0, 1):
                    to = pl.ds(pl.multiple_of((3 - jnp.abs(al - j)) * quarter, quarter), quarter)
                    aT[to, cols] = block[j * quarter:(j + 1) * quarter]
            else:
                aT[:half, cols] = block

            @pl.when(i + LOADS < 2 * blocks)
            def _():
                load_a(n, i + LOADS).start()

    def product(t, first):
        return jnp.dot(aT[first:first + half, :], gbuf[lax.rem(t, 2)], preferred_element_type=F32)

    def copy0(c):
        return rdma(send0.at[lax.rem(c, 2)], recv0.at[lax.rem(c, CREDITS)], s0.at[lax.rem(c, 2)],
                    r0.at[lax.rem(c, CREDITS)], partner)

    def copyA(c):
        return rdma(sendA.at[lax.rem(c, 2)], recvA.at[c], sA.at[lax.rem(c, 2)], rA.at[c], over_A)

    def copyR(c):
        return rdma(sendR.at[lax.rem(c, 2)], at(c, keep, piece), sR.at[lax.rem(c, 2)], rR.at[c], up)

    def copyL(c):
        return rdma(sendL.at[lax.rem(c, 2)], at(c, keep + piece, piece), sL.at[lax.rem(c, 2)], rL.at[c], down)

    def copyB(c):
        return rdma(sendB.at[lax.rem(c, 2)], recvB.at[c], sB.at[lax.rem(c, 2)], rB.at[c], over_B)

    def reuse(c, copy):
        @pl.when(c >= 2)
        def _():
            copy(c - 2).wait_send()

    def give_leaf(c):
        own = at(c, keep + end * piece + be * leaf, leaf)
        return rdma(own, own, gBs, gB.at[c], over_B)

    def take_leaf(c):
        there = at(c, keep + end * piece + (1 - be) * leaf, leaf)
        return rdma(there, there, gBs, gB.at[c], over_B)

    def stage1(c):
        copy0(c).wait_recv()
        reuse(c, copyA)
        for i in (0, piece):
            old = recv0[lax.rem(c, CREDITS), pl.ds(pl.multiple_of((1 - al) * quarter + i, piece), piece), :]
            sendA[lax.rem(c, 2), i:i + piece, :] = (mL[i:i + piece, :] + old.astype(F32)).astype(BF16)
        copyA(c).start()

    def total(c, i):
        old = recv0[lax.rem(c, CREDITS), pl.ds(pl.multiple_of(al * quarter + i, piece), piece), :]
        here = mK[lax.rem(c, KEPT), i:i + piece, :] + old.astype(F32)
        return here + recvA[c, i:i + piece, :].astype(F32)

    def first_hop(c, i, send, copy):
        reuse(c, copy)
        send[lax.rem(c, 2)] = total(c, i).astype(BF16)
        copy(c).start()
        mK[lax.rem(c, KEPT), piece - i:2 * piece - i, :] = total(c, piece - i)

    def stage2(c):
        copyA(c).wait_recv()
        pl.when(z == 0)(lambda: first_hop(c, 0, sendR, copyR))
        pl.when(z == 3)(lambda: first_hop(c, piece, sendL, copyL))

        @pl.when((z == 1) | (z == 2))
        def _():
            for i in (0, piece):
                mK[lax.rem(c, KEPT), i:i + piece, :] = total(c, i)

        @pl.when(c + CREDITS < chunks)
        def _():
            pl.semaphore_signal(credit, inc=1, device_id={"dp": partner}, device_id_type=MESH)

    def pass_on(c, first, send, copy):
        copy(c).wait_recv()
        reuse(c, copy)
        here = mK[lax.rem(c, KEPT), first:first + piece, :]
        send[lax.rem(c, 2)] = (here + o_ref[index(c, keep + first, piece)].astype(F32)).astype(BF16)
        copy(c).start()

    def hop_up(c):
        pass_on(c, 0, sendR, copyR)

    def hop_down(c):
        pass_on(c, piece, sendL, copyL)

    def stage3(c):
        pl.when(z == 1)(lambda: hop_up(c))
        pl.when(z == 2)(lambda: hop_down(c))

    def stage4(c):
        pl.when(z == 2)(lambda: hop_up(c))
        pl.when(z == 1)(lambda: hop_down(c))

    def finish_z(c, first, copy):
        copy(c).wait_recv()
        reuse(c, copyB)
        away = first + (1 - be) * leaf
        total = mK[lax.rem(c, KEPT), pl.ds(pl.multiple_of(away, leaf), leaf), :]
        sendB[lax.rem(c, 2)] = (total + o_ref[index(c, keep + away, leaf)].astype(F32)).astype(BF16)
        copyB(c).start()
        stay = first + be * leaf
        own = pl.ds(pl.multiple_of(stay, leaf), leaf)
        mK[lax.rem(c, KEPT), own, :] += o_ref[index(c, keep + stay, leaf)].astype(F32)

    def stage5(c):
        pl.when(z == 3)(lambda: finish_z(c, 0, copyR))
        pl.when(z == 0)(lambda: finish_z(c, piece, copyL))

    def stage6(c):
        @pl.when(is_end)
        def _():
            copyB(c).wait_recv()
            stay = end * piece + be * leaf
            total = mK[lax.rem(c, KEPT), pl.ds(pl.multiple_of(stay, leaf), leaf), :] + recvB[c].astype(F32)
            o_ref[index(c, keep + stay, leaf)] = total.astype(BF16)
            give_leaf(c).start()

    def to_z(c, d):
        here = at(c, keep + d * piece, piece)
        return rdma(here, here, gZs.at[d], gZ.at[c, d], up if d else down)

    def to_A(c, d):
        here = at(c, keep + d * piece, piece)
        return rdma(here, here, gAs.at[d], gA.at[c, d], over_A)

    def from_A(c, d):
        there = at(c, mine + (1 - al) * quarter + d * piece, piece)
        return rdma(there, there, gNs.at[d], gA.at[c, d], up if d else down)

    def to_core(c):
        here = at(c, mine, half)
        return rdma(here, here, gCs, gC, partner)

    def far(d):
        return z if d else 3 - z

    def have(c, d, hop):
        if hop < 3:
            to_z(c, d).start()
        if hop == 0:
            to_A(c, d).start()
        else:
            pl.when(jnp.logical_not(wide(c)))(lambda: to_A(c, d).start())

    def stage7(hop, c):
        for d in (0, 1):
            @pl.when(far(d) == hop)
            def _(d=d):
                if hop == 0:
                    take_leaf(c).wait_recv()
                else:
                    to_z(c, d).wait_recv()
                have(c, d, hop)

    def stage8(hop, c):
        for d in (0, 1):
            @pl.when(far(d) == hop)
            def _(d=d):
                from_A(c, d).wait_recv()
                if hop < 3:
                    pl.when(wide(c))(lambda: from_A(c, d).start())

        if hop >= 2:
            @pl.when((jnp.maximum(far(0), far(1)) == hop))
            def _():
                to_core(c).start()

    stages = [(S1, stage1), (S2, stage2), (S3, stage3), (S4, stage4), (S5, stage5), (S6, stage6)]
    stages += [(lag, functools.partial(stage7, hop)) for hop, lag in enumerate(S7)]
    stages += [(lag, functools.partial(stage8, hop)) for hop, lag in enumerate(S8)]
    last = max(lag for lag, _ in stages) // 2

    def serve(t, q):
        for lag, f in sorted(stages, key=lambda s: s[0]):
            if lag % 2 == q:
                c = t - lag // 2

                @pl.when((c >= 0) & (c < chunks))
                def _(f=f, c=c):
                    f(c)

    start_a(0)
    load_g(0).start()
    barrier = pltpu.get_barrier_semaphore()
    for other in (partner, over_A, over_B):
        pl.semaphore_signal(barrier, inc=1, device_id={"dp": other}, device_id_type=MESH)

    @pl.when(z < 3)
    def _():
        pl.semaphore_signal(barrier, inc=1, device_id={"dp": up}, device_id_type=MESH)

    @pl.when(z > 0)
    def _():
        pl.semaphore_signal(barrier, inc=1, device_id={"dp": down}, device_id_type=MESH)

    transpose_a(0, 0)
    pl.semaphore_wait(barrier, 3 + (z < 3).astype(jnp.int32) + (z > 0).astype(jnp.int32))

    @pl.loop(0, chunks + last)
    def _(t):
        @pl.when(t + 1 < chunks)
        def _():
            load_g(t + 1).start()

        serve(t, 0)

        @pl.when(t < chunks)
        def _():
            for n in range(1, mats):
                pl.when(t == n * per)(functools.partial(transpose_a, n, 0))
                pl.when(t == n * per - 1)(functools.partial(start_a, n))

            load_g(t).wait()
            reuse(t, copy0)
            send0[lax.rem(t, 2)] = product(t, 0).astype(BF16)

            @pl.when(t >= CREDITS)
            def _():
                pl.semaphore_wait(credit, 1)

            copy0(t).start()

        serve(t, 1)

        @pl.when(t < chunks)
        def _():
            for n in range(mats):
                pl.when(t == n * per)(functools.partial(transpose_a, n, 1))

            both = product(t, half)
            mL[...] = both[:quarter]
            mK[lax.rem(t, KEPT)] = both[quarter:]

    def rest(first, count):
        return o_ref.at[:, pl.ds(pl.multiple_of(first, leaf), count), :]

    for c in range(chunks - 2, chunks):
        copy0(c).wait_send()
        copyA(c).wait_send()
        pl.when(z < 3)(lambda: copyR(c).wait_send())
        pl.when(z > 0)(lambda: copyL(c).wait_send())

        @pl.when(is_end)
        def _(c=c):
            copyB(c).wait_send()

    @pl.when(is_end)
    def _():
        some = rest(keep, leaf)
        rdma(some, some, gBs, gC, over_B).wait_send()

    wides = sum(c % 4 == 2 and c < 22 for c in range(chunks))

    def several(d, count):
        return o_ref.at[:, pl.ds(pl.multiple_of(keep + d * piece, piece), piece), pl.ds(0, count * width // mats)]

    for d in (0, 1):
        @pl.when(far(d) < 3)
        def _(d=d):
            some = several(d, chunks)
            rdma(some, some, gZs.at[d], gC, partner).wait_send()
            some = several(d, wides)
            rdma(some, some, gNs.at[d], gC, partner).wait_send()

        @pl.when(far(d) == 0)
        def _(d=d):
            some = several(d, chunks)
            rdma(some, some, gAs.at[d], gC, over_A).wait_send()

        @pl.when(far(d) > 0)
        def _(d=d):
            some = several(d, chunks - wides)
            rdma(some, some, gAs.at[d], gC, over_A).wait_send()

    some = rest(mine, half)
    rdma(some, some, gCs, gC, partner).wait_send()
    some = rest((1 - core) * half, half)
    rdma(some, some, gCs, gC, partner).wait_recv()


def solution(mesh, width=256, stage=256):
    def step(a, g):
        mats, depth, rows = a.shape[1:]
        columns = g.shape[3]
        chunks = mats * (columns // width)
        half, quarter, piece, leaf = rows // 2, rows // 4, rows // 8, rows // 16
        dma = pltpu.SemaphoreType.DMA
        return pl.pallas_call(
            functools.partial(kernel, width, stage),
            out_shape=pltpu.VMEM((mats, rows, columns), BF16),
            in_specs=[pl.BlockSpec(memory_space=pl.ANY)] * 2,
            out_specs=pl.BlockSpec(memory_space=pltpu.VMEM),
            scratch_shapes=[
                pltpu.VMEM((rows, depth), BF16),
                pltpu.VMEM((LOADS, stage, half), BF16),
                pltpu.VMEM((2, depth, width), BF16),
                pltpu.VMEM((2, half, width), BF16),
                pltpu.VMEM((CREDITS, half, width), BF16),
                pltpu.VMEM((quarter, width), F32),
                pltpu.VMEM((KEPT, quarter, width), F32),
                pltpu.VMEM((2, quarter, width), BF16),
                pltpu.VMEM((chunks, quarter, width), BF16),
                pltpu.VMEM((2, piece, width), BF16),
                pltpu.VMEM((2, piece, width), BF16),
                pltpu.VMEM((2, leaf, width), BF16),
                pltpu.VMEM((chunks, leaf, width), BF16),
                dma((LOADS,)), dma((2,)), dma((2,)), dma((CREDITS,)), dma((2,)), dma((chunks,)), dma((2,)),
                dma((chunks,)), dma((2,)), dma((chunks,)), dma((2,)), dma((chunks,)), dma, dma((chunks,)), dma((2,)),
                dma((chunks, 2)), dma((2,)), dma((2,)), dma((chunks, 2)), dma, dma,
                pltpu.SemaphoreType.REGULAR,
            ],
            compiler_params=pltpu.CompilerParams(collective_id=0, has_side_effects=True, vmem_limit_bytes=40 * 1000 * 1000),
        )(a, g)

    return jax.shard_map(step, mesh=mesh, in_specs=(P(("rep", "dp")), P(("rep", "dp"))), out_specs=P("rep"),
                         check_vma=False)
```

```python
import functools

import jax
import jax.numpy as jnp
from jax import lax
from jax.experimental import pallas as pl
from jax.experimental.pallas import tpu as pltpu
from jax.sharding import PartitionSpec as P

MESH = pl.DeviceIdType.MESH
F32, BF16 = jnp.float32, jnp.bfloat16
CREDITS = 8
KEPT = 16
LOADS = 16
S1, S2, S3, S4, S5, S6 = 2, 5, 8, 11, 14, 17
S7 = 19, 24, 29, 40
S8 = 30, 33, 36, 49


def wide(c):
    return (lax.rem(c, 4) == 2) & (c < 22)


def kernel(width, stage, a_ref, g_ref, o_ref, aT, ast, gbuf, send0, recv0, mL, mK, sendA, recvA, sendR, sendL, sendB,
           recvB, a_sem, g_sem, s0, r0, sA, rA, sR, rR, sL, rL, sB, rB, gBs, gB, gZs, gZ, gNs, gAs, gA, gCs, gC, credit):
    me = lax.axis_index("dp")
    core, z = lax.rem(me, 2), lax.rem(me // 2, 4)
    y, x = lax.rem(me // 8, 2), me // 16
    partner = me + 1 - 2 * core
    over_x, over_y = me + 16 * (1 - 2 * x), me + 8 * (1 - 2 * y)
    over_A = over_x * (1 - core) + over_y * core
    over_B = over_y * (1 - core) + over_x * core
    al, be = x * (1 - core) + y * core, y * (1 - core) + x * core
    up, down = me + 2, me - 2
    mats, depth, rows = a_ref.shape[1:]
    per = g_ref.shape[3] // width
    chunks = mats * per
    half, quarter, piece, leaf = rows // 2, rows // 4, rows // 8, rows // 16
    mine, keep = core * half, core * half + al * quarter
    end = 1 - z // 3
    is_end = (z == 0) | (z == 3)

    def at(c, first, count):
        return o_ref.at[index(c, first, count)]

    def place(c):
        n = c // per if isinstance(c, int) else sum((c >= m * per).astype(jnp.int32) for m in range(1, mats))
        return n, pl.ds(pl.multiple_of((c - n * per) * width, width), width)

    def index(c, first, count):
        n, cols = place(c)
        return n, pl.ds(pl.multiple_of(first, leaf), count), cols

    def rdma(src, dst, ssem, rsem, to):
        return pltpu.make_async_remote_copy(src_ref=src, dst_ref=dst, send_sem=ssem, recv_sem=rsem, device_id={"dp": to},
                                            device_id_type=MESH)

    blocks = depth // stage

    def load_a(n, i):
        late = int(i >= blocks) if isinstance(i, int) else (i >= blocks).astype(jnp.int32)
        k = i - late * blocks
        cols = pl.ds(pl.multiple_of((core * late + (1 - core) * (1 - late)) * half, half), half)
        slot = lax.rem(i, LOADS)
        return pltpu.make_async_copy(a_ref.at[0, n, pl.ds(pl.multiple_of(k * stage, stage), stage), cols], ast.at[slot],
                                     a_sem.at[slot])

    def load_g(t):
        n, cols = place(t)
        return pltpu.make_async_copy(g_ref.at[0, n, :, cols], gbuf.at[lax.rem(t, 2)], g_sem.at[lax.rem(t, 2)])

    def start_a(n):
        for i in range(min(LOADS, 2 * blocks)):
            load_a(n, i).start()

    def transpose_a(n, late):
        @pl.loop(late * blocks, (late + 1) * blocks)
        def _(i):
            load_a(n, i).wait()
            block = ast[lax.rem(i, LOADS)].T
            cols = pl.ds(pl.multiple_of((i - late * blocks) * stage, stage), stage)
            if late:
                for j in (0, 1):
                    to = pl.ds(pl.multiple_of((3 - jnp.abs(al - j)) * quarter, quarter), quarter)
                    aT[to, cols] = block[j * quarter:(j + 1) * quarter]
            else:
                aT[:half, cols] = block

            @pl.when(i + LOADS < 2 * blocks)
            def _():
                load_a(n, i + LOADS).start()

    def product(t, first):
        return jnp.dot(aT[first:first + half, :], gbuf[lax.rem(t, 2)], preferred_element_type=F32)

    def copy0(c):
        return rdma(send0.at[lax.rem(c, 2)], recv0.at[lax.rem(c, CREDITS)], s0.at[lax.rem(c, 2)],
                    r0.at[lax.rem(c, CREDITS)], partner)

    def copyA(c):
        return rdma(sendA.at[lax.rem(c, 2)], recvA.at[c], sA.at[lax.rem(c, 2)], rA.at[c], over_A)

    def copyR(c):
        return rdma(sendR.at[lax.rem(c, 2)], at(c, keep, piece), sR.at[lax.rem(c, 2)], rR.at[c], up)

    def copyL(c):
        return rdma(sendL.at[lax.rem(c, 2)], at(c, keep + piece, piece), sL.at[lax.rem(c, 2)], rL.at[c], down)

    def copyB(c):
        return rdma(sendB.at[lax.rem(c, 2)], recvB.at[c], sB.at[lax.rem(c, 2)], rB.at[c], over_B)

    def reuse(c, copy):
        @pl.when(c >= 2)
        def _():
            copy(c - 2).wait_send()

    def give_leaf(c):
        own = at(c, keep + end * piece + be * leaf, leaf)
        return rdma(own, own, gBs, gB.at[c], over_B)

    def take_leaf(c):
        there = at(c, keep + end * piece + (1 - be) * leaf, leaf)
        return rdma(there, there, gBs, gB.at[c], over_B)

    def stage1(c):
        copy0(c).wait_recv()
        reuse(c, copyA)
        for i in (0, piece):
            old = recv0[lax.rem(c, CREDITS), pl.ds(pl.multiple_of((1 - al) * quarter + i, piece), piece), :]
            sendA[lax.rem(c, 2), i:i + piece, :] = (mL[i:i + piece, :] + old.astype(F32)).astype(BF16)
        copyA(c).start()

    def total(c, i):
        old = recv0[lax.rem(c, CREDITS), pl.ds(pl.multiple_of(al * quarter + i, piece), piece), :]
        here = mK[lax.rem(c, KEPT), i:i + piece, :] + old.astype(F32)
        return here + recvA[c, i:i + piece, :].astype(F32)

    def first_hop(c, i, send, copy):
        reuse(c, copy)
        send[lax.rem(c, 2)] = total(c, i).astype(BF16)
        copy(c).start()
        mK[lax.rem(c, KEPT), piece - i:2 * piece - i, :] = total(c, piece - i)

    def stage2(c):
        copyA(c).wait_recv()
        pl.when(z == 0)(lambda: first_hop(c, 0, sendR, copyR))
        pl.when(z == 3)(lambda: first_hop(c, piece, sendL, copyL))

        @pl.when((z == 1) | (z == 2))
        def _():
            for i in (0, piece):
                mK[lax.rem(c, KEPT), i:i + piece, :] = total(c, i)

        @pl.when(c + CREDITS < chunks)
        def _():
            pl.semaphore_signal(credit, inc=1, device_id={"dp": partner}, device_id_type=MESH)

    def pass_on(c, first, send, copy):
        copy(c).wait_recv()
        reuse(c, copy)
        here = mK[lax.rem(c, KEPT), first:first + piece, :]
        send[lax.rem(c, 2)] = (here + o_ref[index(c, keep + first, piece)].astype(F32)).astype(BF16)
        copy(c).start()

    def hop_up(c):
        pass_on(c, 0, sendR, copyR)

    def hop_down(c):
        pass_on(c, piece, sendL, copyL)

    def stage3(c):
        pl.when(z == 1)(lambda: hop_up(c))
        pl.when(z == 2)(lambda: hop_down(c))

    def stage4(c):
        pl.when(z == 2)(lambda: hop_up(c))
        pl.when(z == 1)(lambda: hop_down(c))

    def finish_z(c, first, copy):
        copy(c).wait_recv()
        reuse(c, copyB)
        away = first + (1 - be) * leaf
        total = mK[lax.rem(c, KEPT), pl.ds(pl.multiple_of(away, leaf), leaf), :]
        sendB[lax.rem(c, 2)] = (total + o_ref[index(c, keep + away, leaf)].astype(F32)).astype(BF16)
        copyB(c).start()
        stay = first + be * leaf
        own = pl.ds(pl.multiple_of(stay, leaf), leaf)
        mK[lax.rem(c, KEPT), own, :] += o_ref[index(c, keep + stay, leaf)].astype(F32)

    def stage5(c):
        pl.when(z == 3)(lambda: finish_z(c, 0, copyR))
        pl.when(z == 0)(lambda: finish_z(c, piece, copyL))

    def stage6(c):
        @pl.when(is_end)
        def _():
            copyB(c).wait_recv()
            stay = end * piece + be * leaf
            total = mK[lax.rem(c, KEPT), pl.ds(pl.multiple_of(stay, leaf), leaf), :] + recvB[c].astype(F32)
            o_ref[index(c, keep + stay, leaf)] = total.astype(BF16)
            give_leaf(c).start()

    def to_z(c, d):
        here = at(c, keep + d * piece, piece)
        return rdma(here, here, gZs.at[d], gZ.at[c, d], up if d else down)

    def to_A(c, d):
        here = at(c, keep + d * piece, piece)
        return rdma(here, here, gAs.at[d], gA.at[c, d], over_A)

    def from_A(c, d):
        there = at(c, mine + (1 - al) * quarter + d * piece, piece)
        return rdma(there, there, gNs.at[d], gA.at[c, d], up if d else down)

    def to_core(c):
        here = at(c, mine, half)
        return rdma(here, here, gCs, gC, partner)

    def far(d):
        return z if d else 3 - z

    def have(c, d, hop):
        if hop < 3:
            to_z(c, d).start()
        if hop == 0:
            to_A(c, d).start()
        else:
            pl.when(jnp.logical_not(wide(c)))(lambda: to_A(c, d).start())

    def stage7(hop, c):
        for d in (0, 1):
            @pl.when(far(d) == hop)
            def _(d=d):
                if hop == 0:
                    take_leaf(c).wait_recv()
                else:
                    to_z(c, d).wait_recv()
                have(c, d, hop)

    def stage8(hop, c):
        for d in (0, 1):
            @pl.when(far(d) == hop)
            def _(d=d):
                from_A(c, d).wait_recv()
                if hop < 3:
                    pl.when(wide(c))(lambda: from_A(c, d).start())

        if hop >= 2:
            @pl.when((jnp.maximum(far(0), far(1)) == hop))
            def _():
                to_core(c).start()

    stages = [(S1, stage1), (S2, stage2), (S3, stage3), (S4, stage4), (S5, stage5), (S6, stage6)]
    stages += [(lag, functools.partial(stage7, hop)) for hop, lag in enumerate(S7)]
    stages += [(lag, functools.partial(stage8, hop)) for hop, lag in enumerate(S8)]
    last = max(lag for lag, _ in stages) // 2

    def serve(t, q):
        for lag, f in sorted(stages, key=lambda s: s[0]):
            if lag % 2 == q:
                c = t - lag // 2

                @pl.when((c >= 0) & (c < chunks))
                def _(f=f, c=c):
                    f(c)

    start_a(0)
    load_g(0).start()
    barrier = pltpu.get_barrier_semaphore()
    for other in (partner, over_A, over_B):
        pl.semaphore_signal(barrier, inc=1, device_id={"dp": other}, device_id_type=MESH)

    @pl.when(z < 3)
    def _():
        pl.semaphore_signal(barrier, inc=1, device_id={"dp": up}, device_id_type=MESH)

    @pl.when(z > 0)
    def _():
        pl.semaphore_signal(barrier, inc=1, device_id={"dp": down}, device_id_type=MESH)

    transpose_a(0, 0)
    pl.semaphore_wait(barrier, 3 + (z < 3).astype(jnp.int32) + (z > 0).astype(jnp.int32))

    @pl.loop(0, chunks + last)
    def _(t):
        @pl.when(t + 1 < chunks)
        def _():
            load_g(t + 1).start()

        serve(t, 0)

        @pl.when(t < chunks)
        def _():
            for n in range(1, mats):
                pl.when(t == n * per)(functools.partial(transpose_a, n, 0))
                pl.when(t == n * per - 1)(functools.partial(start_a, n))

            load_g(t).wait()
            reuse(t, copy0)
            send0[lax.rem(t, 2)] = product(t, 0).astype(BF16)

            @pl.when(t >= CREDITS)
            def _():
                pl.semaphore_wait(credit, 1)

            copy0(t).start()

        serve(t, 1)

        @pl.when(t < chunks)
        def _():
            for n in range(mats):
                pl.when(t == n * per)(functools.partial(transpose_a, n, 1))

            both = product(t, half)
            mL[...] = both[:quarter]
            mK[lax.rem(t, KEPT)] = both[quarter:]

    def rest(first, count):
        return o_ref.at[:, pl.ds(pl.multiple_of(first, leaf), count), :]

    for c in range(chunks - 2, chunks):
        copy0(c).wait_send()
        copyA(c).wait_send()
        pl.when(z < 3)(lambda: copyR(c).wait_send())
        pl.when(z > 0)(lambda: copyL(c).wait_send())

        @pl.when(is_end)
        def _(c=c):
            copyB(c).wait_send()

    @pl.when(is_end)
    def _():
        some = rest(keep, leaf)
        rdma(some, some, gBs, gC, over_B).wait_send()

    wides = sum(c % 4 == 2 and c < 22 for c in range(chunks))

    def several(d, count):
        return o_ref.at[:, pl.ds(pl.multiple_of(keep + d * piece, piece), piece), pl.ds(0, count * width // mats)]

    for d in (0, 1):
        @pl.when(far(d) < 3)
        def _(d=d):
            some = several(d, chunks)
            rdma(some, some, gZs.at[d], gC, partner).wait_send()
            some = several(d, wides)
            rdma(some, some, gNs.at[d], gC, partner).wait_send()

        @pl.when(far(d) == 0)
        def _(d=d):
            some = several(d, chunks)
            rdma(some, some, gAs.at[d], gC, over_A).wait_send()

        @pl.when(far(d) > 0)
        def _(d=d):
            some = several(d, chunks - wides)
            rdma(some, some, gAs.at[d], gC, over_A).wait_send()

    some = rest(mine, half)
    rdma(some, some, gCs, gC, partner).wait_send()
    some = rest((1 - core) * half, half)
    rdma(some, some, gCs, gC, partner).wait_recv()


def solution(mesh, width=256, stage=256):
    def step(a, g):
        mats, depth, rows = a.shape[1:]
        columns = g.shape[3]
        chunks = mats * (columns // width)
        half, quarter, piece, leaf = rows // 2, rows // 4, rows // 8, rows // 16
        dma = pltpu.SemaphoreType.DMA
        return pl.pallas_call(
            functools.partial(kernel, width, stage),
            out_shape=pltpu.VMEM((mats, rows, columns), BF16),
            in_specs=[pl.BlockSpec(memory_space=pl.ANY)] * 2,
            out_specs=pl.BlockSpec(memory_space=pltpu.VMEM),
            scratch_shapes=[
                pltpu.VMEM((rows, depth), BF16),
                pltpu.VMEM((LOADS, stage, half), BF16),
                pltpu.VMEM((2, depth, width), BF16),
                pltpu.VMEM((2, half, width), BF16),
                pltpu.VMEM((CREDITS, half, width), BF16),
                pltpu.VMEM((quarter, width), F32),
                pltpu.VMEM((KEPT, quarter, width), F32),
                pltpu.VMEM((2, quarter, width), BF16),
                pltpu.VMEM((chunks, quarter, width), BF16),
                pltpu.VMEM((2, piece, width), BF16),
                pltpu.VMEM((2, piece, width), BF16),
                pltpu.VMEM((2, leaf, width), BF16),
                pltpu.VMEM((chunks, leaf, width), BF16),
                dma((LOADS,)), dma((2,)), dma((2,)), dma((CREDITS,)), dma((2,)), dma((chunks,)), dma((2,)),
                dma((chunks,)), dma((2,)), dma((chunks,)), dma((2,)), dma((chunks,)), dma, dma((chunks,)), dma((2,)),
                dma((chunks, 2)), dma((2,)), dma((2,)), dma((chunks, 2)), dma, dma,
                pltpu.SemaphoreType.REGULAR,
            ],
            compiler_params=pltpu.CompilerParams(collective_id=0, has_side_effects=True, vmem_limit_bytes=40 * 1000 * 1000),
        )(a, g)

    return jax.shard_map(step, mesh=mesh, in_specs=(P(("rep", "dp")), P(("rep", "dp"))), out_specs=P("rep"),
                         check_vma=False)
```

```python
import functools

import jax
import jax.numpy as jnp
from jax import lax
from jax.experimental import pallas as pl
from jax.experimental.pallas import tpu as pltpu
from jax.sharding import PartitionSpec as P

MESH = pl.DeviceIdType.MESH
F32, BF16 = jnp.float32, jnp.bfloat16
CREDITS = 8
KEPT = 16
LOADS = 16
S1, S2, S3, S4, S5, S6 = 2, 5, 8, 11, 14, 17
S7 = 20, 25, 30, 41
S8 = 30, 35, 38, 52
ORDER = 3, 7, 9, 11, 0, 1, 8, 13, 4, 10, 6, 12, 5, 2


def wide(c):
    return (lax.rem(c, 4) == 2) & (c < 22)


def kernel(width, stage, a_ref, g_ref, o_ref, aT, ast, gbuf, send0, recv0, mL, mK, sendA, recvA, sendR, sendL, sendB,
           recvB, a_sem, g_sem, s0, r0, sA, rA, sR, rR, sL, rL, sB, rB, gBs, gB, gZs, gZ, gNs, gAs, gA, gCs, gC, credit):
    me = lax.axis_index("dp")
    core, z = lax.rem(me, 2), lax.rem(me // 2, 4)
    y, x = lax.rem(me // 8, 2), me // 16
    partner = me + 1 - 2 * core
    over_x, over_y = me + 16 * (1 - 2 * x), me + 8 * (1 - 2 * y)
    over_A = over_x * (1 - core) + over_y * core
    over_B = over_y * (1 - core) + over_x * core
    al, be = x * (1 - core) + y * core, y * (1 - core) + x * core
    up, down = me + 2, me - 2
    mats, depth, rows = a_ref.shape[1:]
    per = g_ref.shape[3] // width
    chunks = mats * per
    half, quarter, piece, leaf = rows // 2, rows // 4, rows // 8, rows // 16
    mine, keep = core * half, core * half + al * quarter
    end = 1 - z // 3
    is_end = (z == 0) | (z == 3)

    def at(c, first, count):
        return o_ref.at[index(c, first, count)]

    def place(c):
        n = c // per if isinstance(c, int) else sum((c >= m * per).astype(jnp.int32) for m in range(1, mats))
        return n, pl.ds(pl.multiple_of((c - n * per) * width, width), width)

    def index(c, first, count):
        n, cols = place(c)
        return n, pl.ds(pl.multiple_of(first, leaf), count), cols

    def rdma(src, dst, ssem, rsem, to):
        return pltpu.make_async_remote_copy(src_ref=src, dst_ref=dst, send_sem=ssem, recv_sem=rsem, device_id={"dp": to},
                                            device_id_type=MESH)

    blocks = depth // stage

    def load_a(n, i):
        late = int(i >= blocks) if isinstance(i, int) else (i >= blocks).astype(jnp.int32)
        k = i - late * blocks
        cols = pl.ds(pl.multiple_of((core * late + (1 - core) * (1 - late)) * half, half), half)
        slot = lax.rem(i, LOADS)
        return pltpu.make_async_copy(a_ref.at[0, n, pl.ds(pl.multiple_of(k * stage, stage), stage), cols], ast.at[slot],
                                     a_sem.at[slot])

    def load_g(t):
        n, cols = place(t)
        return pltpu.make_async_copy(g_ref.at[0, n, :, cols], gbuf.at[lax.rem(t, 2)], g_sem.at[lax.rem(t, 2)])

    def start_a(n):
        for i in range(min(LOADS, 2 * blocks)):
            load_a(n, i).start()

    def transpose_a(n, late):
        @pl.loop(late * blocks, (late + 1) * blocks)
        def _(i):
            load_a(n, i).wait()
            block = ast[lax.rem(i, LOADS)].T
            cols = pl.ds(pl.multiple_of((i - late * blocks) * stage, stage), stage)
            if late:
                for j in (0, 1):
                    to = pl.ds(pl.multiple_of((3 - jnp.abs(al - j)) * quarter, quarter), quarter)
                    aT[to, cols] = block[j * quarter:(j + 1) * quarter]
            else:
                aT[:half, cols] = block

            @pl.when(i + LOADS < 2 * blocks)
            def _():
                load_a(n, i + LOADS).start()

    def product(t, first):
        return jnp.dot(aT[first:first + half, :], gbuf[lax.rem(t, 2)], preferred_element_type=F32)

    def copy0(c):
        return rdma(send0.at[lax.rem(c, 2)], recv0.at[lax.rem(c, CREDITS)], s0.at[lax.rem(c, 2)],
                    r0.at[lax.rem(c, CREDITS)], partner)

    def copyA(c):
        return rdma(sendA.at[lax.rem(c, 2)], recvA.at[c], sA.at[lax.rem(c, 2)], rA.at[c], over_A)

    def copyR(c):
        return rdma(sendR.at[lax.rem(c, 2)], at(c, keep, piece), sR.at[lax.rem(c, 2)], rR.at[c], up)

    def copyL(c):
        return rdma(sendL.at[lax.rem(c, 2)], at(c, keep + piece, piece), sL.at[lax.rem(c, 2)], rL.at[c], down)

    def copyB(c):
        return rdma(sendB.at[lax.rem(c, 2)], recvB.at[c], sB.at[lax.rem(c, 2)], rB.at[c], over_B)

    def reuse(c, copy):
        @pl.when(c >= 2)
        def _():
            copy(c - 2).wait_send()

    def give_leaf(c):
        own = at(c, keep + end * piece + be * leaf, leaf)
        return rdma(own, own, gBs, gB.at[c], over_B)

    def take_leaf(c):
        there = at(c, keep + end * piece + (1 - be) * leaf, leaf)
        return rdma(there, there, gBs, gB.at[c], over_B)

    def stage1(c):
        copy0(c).wait_recv()
        reuse(c, copyA)
        for i in (0, piece):
            old = recv0[lax.rem(c, CREDITS), pl.ds(pl.multiple_of((1 - al) * quarter + i, piece), piece), :]
            sendA[lax.rem(c, 2), i:i + piece, :] = (mL[i:i + piece, :] + old.astype(F32)).astype(BF16)
        copyA(c).start()

    def total(c, i):
        old = recv0[lax.rem(c, CREDITS), pl.ds(pl.multiple_of(al * quarter + i, piece), piece), :]
        here = mK[lax.rem(c, KEPT), i:i + piece, :] + old.astype(F32)
        return here + recvA[c, i:i + piece, :].astype(F32)

    def first_hop(c, i, send, copy):
        reuse(c, copy)
        send[lax.rem(c, 2)] = total(c, i).astype(BF16)
        copy(c).start()
        mK[lax.rem(c, KEPT), piece - i:2 * piece - i, :] = total(c, piece - i)

    def stage2(c):
        copyA(c).wait_recv()
        pl.when(z == 0)(lambda: first_hop(c, 0, sendR, copyR))
        pl.when(z == 3)(lambda: first_hop(c, piece, sendL, copyL))

        @pl.when((z == 1) | (z == 2))
        def _():
            for i in (0, piece):
                mK[lax.rem(c, KEPT), i:i + piece, :] = total(c, i)

        @pl.when(c + CREDITS < chunks)
        def _():
            pl.semaphore_signal(credit, inc=1, device_id={"dp": partner}, device_id_type=MESH)

    def pass_on(c, first, send, copy):
        copy(c).wait_recv()
        reuse(c, copy)
        here = mK[lax.rem(c, KEPT), first:first + piece, :]
        send[lax.rem(c, 2)] = (here + o_ref[index(c, keep + first, piece)].astype(F32)).astype(BF16)
        copy(c).start()

    def hop_up(c):
        pass_on(c, 0, sendR, copyR)

    def hop_down(c):
        pass_on(c, piece, sendL, copyL)

    def stage3(c):
        pl.when(z == 1)(lambda: hop_up(c))
        pl.when(z == 2)(lambda: hop_down(c))

    def stage4(c):
        pl.when(z == 2)(lambda: hop_up(c))
        pl.when(z == 1)(lambda: hop_down(c))

    def finish_z(c, first, copy):
        copy(c).wait_recv()
        reuse(c, copyB)
        away = first + (1 - be) * leaf
        total = mK[lax.rem(c, KEPT), pl.ds(pl.multiple_of(away, leaf), leaf), :]
        sendB[lax.rem(c, 2)] = (total + o_ref[index(c, keep + away, leaf)].astype(F32)).astype(BF16)
        copyB(c).start()
        stay = first + be * leaf
        own = pl.ds(pl.multiple_of(stay, leaf), leaf)
        mK[lax.rem(c, KEPT), own, :] += o_ref[index(c, keep + stay, leaf)].astype(F32)

    def stage5(c):
        pl.when(z == 3)(lambda: finish_z(c, 0, copyR))
        pl.when(z == 0)(lambda: finish_z(c, piece, copyL))

    def stage6(c):
        @pl.when(is_end)
        def _():
            copyB(c).wait_recv()
            stay = end * piece + be * leaf
            total = mK[lax.rem(c, KEPT), pl.ds(pl.multiple_of(stay, leaf), leaf), :] + recvB[c].astype(F32)
            o_ref[index(c, keep + stay, leaf)] = total.astype(BF16)
            give_leaf(c).start()

    def to_z(c, d):
        here = at(c, keep + d * piece, piece)
        return rdma(here, here, gZs.at[d], gZ.at[c, d], up if d else down)

    def to_A(c, d):
        here = at(c, keep + d * piece, piece)
        return rdma(here, here, gAs.at[d], gA.at[c, d], over_A)

    def from_A(c, d):
        there = at(c, mine + (1 - al) * quarter + d * piece, piece)
        return rdma(there, there, gNs.at[d], gA.at[c, d], up if d else down)

    def to_core(c):
        here = at(c, mine, half)
        return rdma(here, here, gCs, gC, partner)

    def far(d):
        return z if d else 3 - z

    def have(c, d, hop):
        if hop < 3:
            to_z(c, d).start()
        if hop == 0:
            to_A(c, d).start()
        else:
            pl.when(jnp.logical_not(wide(c)))(lambda: to_A(c, d).start())

    def stage7(hop, c):
        for d in (0, 1):
            @pl.when(far(d) == hop)
            def _(d=d):
                if hop == 0:
                    take_leaf(c).wait_recv()
                else:
                    to_z(c, d).wait_recv()
                have(c, d, hop)

    def stage8(hop, c):
        for d in (0, 1):
            @pl.when(far(d) == hop)
            def _(d=d):
                from_A(c, d).wait_recv()
                if hop < 3:
                    pl.when(wide(c))(lambda: from_A(c, d).start())

        if hop >= 2:
            @pl.when((jnp.maximum(far(0), far(1)) == hop))
            def _():
                to_core(c).start()

    stages = [(S1, stage1), (S2, stage2), (S3, stage3), (S4, stage4), (S5, stage5), (S6, stage6)]
    stages += [(lag, functools.partial(stage7, hop)) for hop, lag in enumerate(S7)]
    stages += [(lag, functools.partial(stage8, hop)) for hop, lag in enumerate(S8)]
    last = max(lag for lag, _ in stages) // 2

    def serve(t, q):
        for lag, f in (stages[i] for i in ORDER):
            if lag % 2 == q:
                c = t - lag // 2

                @pl.when((c >= 0) & (c < chunks))
                def _(f=f, c=c):
                    f(c)

    start_a(0)
    load_g(0).start()
    barrier = pltpu.get_barrier_semaphore()
    for other in (partner, over_A, over_B):
        pl.semaphore_signal(barrier, inc=1, device_id={"dp": other}, device_id_type=MESH)

    @pl.when(z < 3)
    def _():
        pl.semaphore_signal(barrier, inc=1, device_id={"dp": up}, device_id_type=MESH)

    @pl.when(z > 0)
    def _():
        pl.semaphore_signal(barrier, inc=1, device_id={"dp": down}, device_id_type=MESH)

    transpose_a(0, 0)
    pl.semaphore_wait(barrier, 3 + (z < 3).astype(jnp.int32) + (z > 0).astype(jnp.int32))

    @pl.loop(0, chunks + last)
    def _(t):
        @pl.when(t + 1 < chunks)
        def _():
            load_g(t + 1).start()

        serve(t, 0)

        @pl.when(t < chunks)
        def _():
            for n in range(1, mats):
                pl.when(t == n * per)(functools.partial(transpose_a, n, 0))
                pl.when(t == n * per - 1)(functools.partial(start_a, n))

            load_g(t).wait()
            reuse(t, copy0)
            send0[lax.rem(t, 2)] = product(t, 0).astype(BF16)

            @pl.when(t >= CREDITS)
            def _():
                pl.semaphore_wait(credit, 1)

            copy0(t).start()

        serve(t, 1)

        @pl.when(t < chunks)
        def _():
            for n in range(mats):
                pl.when(t == n * per)(functools.partial(transpose_a, n, 1))

            both = product(t, half)
            mL[...] = both[:quarter]
            mK[lax.rem(t, KEPT)] = both[quarter:]

    def rest(first, count):
        return o_ref.at[:, pl.ds(pl.multiple_of(first, leaf), count), :]

    for c in range(chunks - 2, chunks):
        copy0(c).wait_send()
        copyA(c).wait_send()
        pl.when(z < 3)(lambda: copyR(c).wait_send())
        pl.when(z > 0)(lambda: copyL(c).wait_send())

        @pl.when(is_end)
        def _(c=c):
            copyB(c).wait_send()

    @pl.when(is_end)
    def _():
        some = rest(keep, leaf)
        rdma(some, some, gBs, gC, over_B).wait_send()

    wides = sum(c % 4 == 2 and c < 22 for c in range(chunks))

    def several(d, count):
        return o_ref.at[:, pl.ds(pl.multiple_of(keep + d * piece, piece), piece), pl.ds(0, count * width // mats)]

    for d in (0, 1):
        @pl.when(far(d) < 3)
        def _(d=d):
            some = several(d, chunks)
            rdma(some, some, gZs.at[d], gC, partner).wait_send()
            some = several(d, wides)
            rdma(some, some, gNs.at[d], gC, partner).wait_send()

        @pl.when(far(d) == 0)
        def _(d=d):
            some = several(d, chunks)
            rdma(some, some, gAs.at[d], gC, over_A).wait_send()

        @pl.when(far(d) > 0)
        def _(d=d):
            some = several(d, chunks - wides)
            rdma(some, some, gAs.at[d], gC, over_A).wait_send()

    some = rest(mine, half)
    rdma(some, some, gCs, gC, partner).wait_send()
    some = rest((1 - core) * half, half)
    rdma(some, some, gCs, gC, partner).wait_recv()


def solution(mesh, width=256, stage=256):
    def step(a, g):
        mats, depth, rows = a.shape[1:]
        columns = g.shape[3]
        chunks = mats * (columns // width)
        half, quarter, piece, leaf = rows // 2, rows // 4, rows // 8, rows // 16
        dma = pltpu.SemaphoreType.DMA
        return pl.pallas_call(
            functools.partial(kernel, width, stage),
            out_shape=pltpu.VMEM((mats, rows, columns), BF16),
            in_specs=[pl.BlockSpec(memory_space=pl.ANY)] * 2,
            out_specs=pl.BlockSpec(memory_space=pltpu.VMEM),
            scratch_shapes=[
                pltpu.VMEM((rows, depth), BF16),
                pltpu.VMEM((LOADS, stage, half), BF16),
                pltpu.VMEM((2, depth, width), BF16),
                pltpu.VMEM((2, half, width), BF16),
                pltpu.VMEM((CREDITS, half, width), BF16),
                pltpu.VMEM((quarter, width), F32),
                pltpu.VMEM((KEPT, quarter, width), F32),
                pltpu.VMEM((2, quarter, width), BF16),
                pltpu.VMEM((chunks, quarter, width), BF16),
                pltpu.VMEM((2, piece, width), BF16),
                pltpu.VMEM((2, piece, width), BF16),
                pltpu.VMEM((2, leaf, width), BF16),
                pltpu.VMEM((chunks, leaf, width), BF16),
                dma((LOADS,)), dma((2,)), dma((2,)), dma((CREDITS,)), dma((2,)), dma((chunks,)), dma((2,)),
                dma((chunks,)), dma((2,)), dma((chunks,)), dma((2,)), dma((chunks,)), dma, dma((chunks,)), dma((2,)),
                dma((chunks, 2)), dma((2,)), dma((2,)), dma((chunks, 2)), dma, dma,
                pltpu.SemaphoreType.REGULAR,
            ],
            compiler_params=pltpu.CompilerParams(collective_id=0, has_side_effects=True, vmem_limit_bytes=40 * 1000 * 1000),
        )(a, g)

    return jax.shard_map(step, mesh=mesh, in_specs=(P(("rep", "dp")), P(("rep", "dp"))), out_specs=P("rep"),
                         check_vma=False)
```
